32 devices in a mesh: seq: 16 (over z, y, x), blk: 2 (over core).
Axes of the slice: x: 2, y: 2, z: 4, core: 2. Of those that a mesh axis runs over, the one named last changes fastest.
Arguments:
- query: bfloat16 [2048, 5120], P(('blk', 'seq')), may hold values from -139 to 139
- keys: bfloat16 [2048, 5120], P(('blk', 'seq')), may hold values from -4.5 to 4.5
- values: bfloat16 [2048, 5120], P(('blk', 'seq')), may hold values from -6 to 6
Outputs:
- attended: bfloat16 [2048, 5120], P(('blk', 'seq'))
The draws below stay inside these ranges and needn't reach their ends.
All inputs are finite; a program needn't handle non-finite values.
Results may differ from the reference program's by a relative error of at most 0.008.
Values may be sent and summed in bfloat16 or wider, within the bound.
No kernel may reach another device: no remote copies, remote signals or barrier semaphores. Data moves between devices by JAX's collectives and lax.ppermute only.
A program may use at most 64 MiB of HBM per device.

```python
import jax
import jax.numpy as jnp
from jax import lax

HEADS = 40
HEAD_DIM = 128
SEQ_LEN = 2048


def joint_draw(key):
    base = jax.random.fold_in(key, 7)
    first, second = jax.random.split(base, 2)
    shape = (SEQ_LEN, HEADS * HEAD_DIM)
    keys = jnp.clip(jax.random.normal(first, shape, jnp.float32), -4.5, 4.5)
    query = jnp.clip(jax.random.normal(second, shape, jnp.float32), -4.5, 4.5)
    return (query, keys)


def draw_query(key, part):
    return joint_draw(key)[0].astype(jnp.bfloat16)


def draw_keys(key, part):
    return joint_draw(key)[1].astype(jnp.bfloat16)


def level_of(own_key, shape, pieces, smallest, top_value):
    level = 1.0
    for axis_at, parts in pieces:
        heights = jax.random.uniform(jax.random.fold_in(jax.random.fold_in(own_key, 6), axis_at), (parts,), jnp.float32, smallest / len(pieces), top_value / len(pieces))
        level = level * jnp.repeat(jnp.exp(heights), shape[axis_at] // parts).reshape((-1,) + (1,) * (len(shape) - 1 - axis_at))
    return level


def scatter_about(rng, extent, scale, reach, cuts=(), held_as=jnp.bfloat16):
    factor_of = level_of(rng, extent, cuts, -0.22, 0.18) if cuts else 1.0
    values = jax.random.normal(rng, extent, jnp.float32) * scale * factor_of
    return jnp.minimum(jnp.maximum(values, -reach), reach).astype(held_as)


def setup_inputs(seed: int = 0) -> dict:
    splits = jax.random.split(jax.random.key(seed), 4)
    return {
        "query": draw_query(jax.random.fold_in(splits[3], 71), 0),
        "keys": draw_keys(jax.random.fold_in(splits[3], 71), 0),
        "values": scatter_about(splits[2], (SEQ_LEN, HEADS * HEAD_DIM), 1.0, 6.0, ((0, 32),)),
    }


def reference(query, keys, values):
    length = query.shape[0]
    width = HEAD_DIM
    rows = min(512, length)

    def heads_first(array):
        return jnp.transpose(array.reshape(length, HEADS, width), (1, 0, 2))

    def one_head(args):
        q_head, k_head, v_head = args

        def block(q_rows):
            scores = lax.dot_general(q_rows, k_head, (((1,), (1,)), ((), ())), preferred_element_type=jnp.float32) * (width ** -0.5)
            peak = jnp.max(scores, axis=1, keepdims=True)
            expo = jnp.exp(scores - peak)
            totals = jnp.sum(expo, axis=1)
            summed = jnp.dot(expo.astype(jnp.bfloat16), v_head, preferred_element_type=jnp.float32)
            return (summed / totals[:, None]).astype(jnp.bfloat16)

        return lax.map(block, q_head.reshape(length // rows, rows, width)).reshape(length, width)

    result = lax.map(one_head, (heads_first(query), heads_first(keys), heads_first(values)))
    return jnp.transpose(result, (1, 0, 2)).reshape(length, HEADS * width)
```

```python
import functools
import math

import jax
import jax.numpy as jnp
from jax import lax
from jax.experimental import pallas as pl
from jax.sharding import PartitionSpec as P

HEADS = 40
LOG2E = 1.4426950408889634
KEY_TILE = 1024


def partner(value, axis, mask):
    pairs = [(source, source ^ mask) for source in range(lax.axis_size(axis))]
    return lax.ppermute(value, axis, pairs)


def attention_kernel(*refs):
    q_ref, o_ref = refs[0], refs[-1]
    kv_refs = refs[1:-1]
    width = q_ref.shape[-1]
    q_rows = q_ref[...].reshape(-1, width)
    factor = width ** (-0.5) * LOG2E
    peak = None
    for k_ref, v_ref in zip(kv_refs[0::2], kv_refs[1::2]):
        step = max(1, KEY_TILE // k_ref.shape[-2])
        for at in range(0, k_ref.shape[0], step):
            k_tile = k_ref[at : at + step].reshape(-1, width)
            v_tile = v_ref[at : at + step].reshape(-1, width)
            scores = lax.dot_general(
                q_rows, k_tile, (((1,), (1,)), ((), ())), preferred_element_type=jnp.float32
            )
            tile_peak = jnp.max(scores, axis=1, keepdims=True)
            if peak is None:
                peak = tile_peak
                expo = jnp.exp2((scores - peak) * factor)
                totals = jnp.sum(expo, axis=1, keepdims=True)
                summed = jnp.dot(
                    expo.astype(jnp.bfloat16), v_tile, preferred_element_type=jnp.float32
                )
            else:
                new_peak = jnp.maximum(peak, tile_peak)
                keep = jnp.exp2((peak - new_peak) * factor)
                peak = new_peak
                expo = jnp.exp2((scores - peak) * factor)
                totals = totals * keep + jnp.sum(expo, axis=1, keepdims=True)
                summed = summed * keep + jnp.dot(
                    expo.astype(jnp.bfloat16), v_tile, preferred_element_type=jnp.float32
                )
    o_ref[...] = (summed / totals).astype(jnp.bfloat16).reshape(o_ref.shape)


def attend(own, others):
    sources, _, count, rows, width = own.shape

    def item(array, index):
        return pl.BlockSpec(
            (array.shape[0], pl.squeezed, pl.squeezed, rows, width),
            lambda head: (0, index, head, 0, 0),
        )

    operands, specs = [own, own, own], [item(own, 0), item(own, 1), item(own, 2)]
    for other in others:
        base = other.shape[1] - 2
        operands += [other, other]
        specs += [item(other, base), item(other, base + 1)]
    return pl.pallas_call(
        attention_kernel,
        grid=(count,),
        in_specs=specs,
        out_specs=pl.BlockSpec(
            (sources, pl.squeezed, rows, width), lambda head: (0, head, 0, 0)
        ),
        out_shape=jax.ShapeDtypeStruct((sources, count, rows, width), jnp.bfloat16),
    )(*operands)


def on_device(query, keys, values):
    devices = lax.axis_size("seq")
    rows = query.shape[0]
    width = query.shape[1] // HEADS
    groups = math.gcd(HEADS, devices)
    members = devices // groups
    in_group = HEADS // groups
    whole = in_group // members
    shared = in_group - whole * members
    columns = [[g * members + m for g in range(groups)] for m in range(members)]

    def by_group(array):
        return array.reshape(rows, groups, in_group, width)

    arrays = [by_group(array) for array in (query, keys, values)]
    results = []
    if whole:
        own = jnp.stack(
            [
                array[:, :, : whole * members].reshape(rows, devices, whole, width)
                for array in arrays
            ]
        )
        own = jnp.transpose(own, (2, 0, 3, 1, 4))
        main = lax.all_to_all(own, "seq", split_axis=0, concat_axis=0, tiled=True)
    if shared:
        part = jnp.stack([array[:, :, whole * members :] for array in arrays])
        part = jnp.transpose(part, (2, 0, 3, 1, 4))
        part = lax.all_to_all(
            part, "seq", split_axis=0, concat_axis=0, tiled=True, axis_index_groups=columns
        )
    if whole:
        main_other = partner(main, "blk", 1)
        main_out = attend(main, [main_other])
    if shared:
        gathered = [part[:, 1:]]
        for step in range(1, members):
            pairs = [
                (g * members + m, g * members + (m + step) % members)
                for g in range(groups)
                for m in range(members)
            ]
            gathered.append(lax.ppermute(gathered[0], "seq", pairs))
        far = partner(jnp.stack(gathered), "blk", 1)
        part_out = attend(part, gathered[1:] + [far[i] for i in range(members)])
    if whole:
        back = lax.all_to_all(main_out, "seq", split_axis=0, concat_axis=0, tiled=True)
        back = back.reshape(groups, members, whole, rows, width)
        results.append(back.reshape(groups, members * whole, rows, width))
    if shared:
        results.append(
            lax.all_to_all(
                part_out, "seq", split_axis=0, concat_axis=0, tiled=True, axis_index_groups=columns
            )
        )
    result = jnp.concatenate(results, axis=1) if len(results) > 1 else results[0]
    return jnp.transpose(result, (2, 0, 1, 3)).reshape(rows, HEADS * width)


def solution(mesh):
    placed = (P(("blk", "seq"), None), P(("blk", "seq"), None), P(("blk", "seq"), None))
    return jax.shard_map(
        on_device, mesh=mesh, in_specs=placed, out_specs=P(("blk", "seq"), None), check_vma=False
    )
```

```python
import functools
import math

import jax
import jax.numpy as jnp
from jax import lax
from jax.experimental import pallas as pl
from jax.sharding import PartitionSpec as P

HEADS = 40
LOG2E = 1.4426950408889634
KEY_TILE = 1024


def partner(value, axis, mask):
    pairs = [(source, source ^ mask) for source in range(lax.axis_size(axis))]
    return lax.ppermute(value, axis, pairs)


def attention_kernel(*refs):
    q_ref, o_ref = refs[0], refs[-1]
    kv_refs = refs[1:-1]
    width = q_ref.shape[-1]
    q_rows = q_ref[...].reshape(-1, width)
    factor = width ** (-0.5) * LOG2E
    peak = None
    for k_ref, v_ref in zip(kv_refs[0::2], kv_refs[1::2]):
        step = max(1, KEY_TILE // k_ref.shape[-2])
        for at in range(0, k_ref.shape[0], step):
            k_tile = k_ref[at : at + step].reshape(-1, width)
            v_tile = v_ref[at : at + step].reshape(-1, width)
            scores = lax.dot_general(
                q_rows, k_tile, (((1,), (1,)), ((), ())), preferred_element_type=jnp.float32
            )
            tile_peak = jnp.max(scores, axis=1, keepdims=True)
            if peak is None:
                peak = tile_peak
                expo = jnp.exp2((scores - peak) * factor)
                totals = jnp.sum(expo, axis=1, keepdims=True)
                summed = jnp.dot(
                    expo.astype(jnp.bfloat16), v_tile, preferred_element_type=jnp.float32
                )
            else:
                new_peak = jnp.maximum(peak, tile_peak)
                keep = jnp.exp2((peak - new_peak) * factor)
                peak = new_peak
                expo = jnp.exp2((scores - peak) * factor)
                totals = totals * keep + jnp.sum(expo, axis=1, keepdims=True)
                summed = summed * keep + jnp.dot(
                    expo.astype(jnp.bfloat16), v_tile, preferred_element_type=jnp.float32
                )
    o_ref[...] = (summed / totals).astype(jnp.bfloat16).reshape(o_ref.shape)


def attend(own, others):
    sources, _, count, rows, width = own.shape

    def item(array, index):
        return pl.BlockSpec(
            (array.shape[0], pl.squeezed, pl.squeezed, rows, width),
            lambda head: (0, index, head, 0, 0),
        )

    operands, specs = [own, own, own], [item(own, 0), item(own, 1), item(own, 2)]
    for other in others:
        base = other.shape[1] - 2
        operands += [other, other]
        specs += [item(other, base), item(other, base + 1)]
    return pl.pallas_call(
        attention_kernel,
        grid=(count,),
        in_specs=specs,
        out_specs=pl.BlockSpec(
            (sources, pl.squeezed, rows, width), lambda head: (0, head, 0, 0)
        ),
        out_shape=jax.ShapeDtypeStruct((sources, count, rows, width), jnp.bfloat16),
    )(*operands)


def pack_kernel(query_ref, keys_ref, values_ref, *out_refs, plan):
    refs = (query_ref, keys_ref, values_ref)
    width = out_refs[0].shape[-1]
    for out_ref, slots in zip(out_refs, plan(out_refs)):
        for slot, block in slots:
            count = out_ref.shape[-3]
            for item, ref in enumerate(refs):
                for head in range(count):
                    at = (block + head) * width
                    if not isinstance(at, int):
                        at = pl.multiple_of(at, width)
                    out_ref[slot, item, head] = ref[:, pl.ds(at, width)]


def unpack_kernel(*refs, places):
    out_ref = refs[-1]
    width = refs[0].shape[-1]
    for ref, slots in zip(refs[:-1], places()):
        for slot, block in slots:
            for head in range(ref.shape[1]):
                at = (block + head) * width
                if not isinstance(at, int):
                    at = pl.multiple_of(at, width)
                out_ref[:, pl.ds(at, width)] = ref[slot, head]


def on_device(query, keys, values):
    devices = lax.axis_size("seq")
    rows = query.shape[0]
    width = query.shape[1] // HEADS
    groups = math.gcd(HEADS, devices)
    members = devices // groups
    in_group = HEADS // groups
    whole = in_group // members
    shared = in_group - whole * members
    dtype = query.dtype
    me = lax.axis_index("seq")
    xor = groups & (groups - 1) == 0

    def away(k, group):
        return group ^ k if xor else (group + k) % groups

    def back_from(k, group):
        return group ^ k if xor else (group + groups - k) % groups

    def to_group(k, step_of):
        return [
            (g * members + m, step_of(k, g) * members + m)
            for g in range(groups)
            for m in range(members)
        ]

    def plan(out_refs):
        group = lax.axis_index("seq") // members
        rest = list(out_refs)
        slots = []
        if whole:
            slots.append(
                [
                    (g * members + m, g * in_group + m * whole)
                    for g in range(groups)
                    for m in range(members)
                ]
            )
        if shared:
            for k in range(groups):
                slots.append([(0, away(k, group) * in_group + members * whole)])
        return slots

    packed = pl.pallas_call(
        functools.partial(pack_kernel, plan=plan),
        out_shape=[
            jax.ShapeDtypeStruct((devices, 3, whole, rows, width), dtype)
        ] * (whole > 0)
        + [jax.ShapeDtypeStruct((1, 3, shared, rows, width), dtype)] * (groups if shared else 0),
    )(query, keys, values)
    if whole:
        main = lax.all_to_all(packed[0], "seq", split_axis=0, concat_axis=0, tiled=True)
    if shared:
        sends = packed[-groups:]
        parts = [sends[0]] + [
            lax.ppermute(sends[k], "seq", to_group(k, away)) for k in range(1, groups)
        ]
    if whole:
        main_other = partner(main, "blk", 1)
        main_out = attend(main, [main_other])
    if shared:
        part = jnp.concatenate(parts)
        gathered = [part[:, 1:]]
        for step in range(1, members):
            pairs = [
                (g * members + m, g * members + (m + step) % members)
                for g in range(groups)
                for m in range(members)
            ]
            gathered.append(lax.ppermute(gathered[0], "seq", pairs))
        far = partner(jnp.stack(gathered), "blk", 1)
        part_out = attend(part, gathered[1:] + [far[i] for i in range(members)])
    finals = []
    if whole:
        finals.append(lax.all_to_all(main_out, "seq", split_axis=0, concat_axis=0, tiled=True))
    if shared:
        finals.append(part_out[:1])
        for k in range(1, groups):
            finals.append(lax.ppermute(part_out[k : k + 1], "seq", to_group(k, back_from)))

    def places():
        group = lax.axis_index("seq") // members
        slots = []
        if whole:
            slots.append(
                [
                    (g * members + m, g * in_group + m * whole)
                    for g in range(groups)
                    for m in range(members)
                ]
            )
        if shared:
            for k in range(groups):
                slots.append([(0, away(k, group) * in_group + members * whole)])
        return slots

    return pl.pallas_call(
        functools.partial(unpack_kernel, places=places),
        out_shape=jax.ShapeDtypeStruct((rows, HEADS * width), dtype),
    )(*finals)


def solution(mesh):
    placed = (P(("blk", "seq"), None), P(("blk", "seq"), None), P(("blk", "seq"), None))
    return jax.shard_map(
        on_device, mesh=mesh, in_specs=placed, out_specs=P(("blk", "seq"), None), check_vma=False
    )
```
